32 devices in a mesh: seq: 8 (over y, x, core), tp: 4 (over z).
Axes of the slice: x: 2, y: 2, z: 4, core: 2. Of those that a mesh axis runs over, the one named last changes fastest.
Arguments:
- queries: bfloat16 [4096, 8192], P('seq', 'tp'), may hold values from -6 to 6
- keys: bfloat16 [4096, 8192], P('seq', 'tp'), may hold values from -0.5 to 0.5
- values: bfloat16 [4096, 8192], P('seq', 'tp'), may hold values from -6 to 6
- gate: bfloat16 [4096, 8192], P('seq', 'tp'), may hold values from -6 to 6
- log_decay: float32 [4096, 64], P('seq', 'tp'), may hold values from -0.8 to 0
- out_grad: bfloat16 [4096, 8192], P('seq', 'tp'), may hold values from -6 to 6
Outputs:
- output: bfloat16 [4096, 8192], P('seq', 'tp')
- query_grad: bfloat16 [4096, 8192], P('seq', 'tp')
- key_grad: bfloat16 [4096, 8192], P('seq', 'tp')
- value_grad: bfloat16 [4096, 8192], P('seq', 'tp')
- gate_grad: bfloat16 [4096, 8192], P('seq', 'tp')
The draws below stay inside these ranges and needn't reach their ends.
All inputs are finite; a program needn't handle non-finite values.
Results may differ from the reference program's by a relative error of at most 0.0051.
Values sent between devices are 32-bit elements; how exact they have to be, the bound alone decides.
A program may use at most 128 MiB of HBM per device.

```python
import jax
import jax.numpy as jnp
from jax import lax

HEAD_COUNT = 64
HEAD = 128
TOK_DEV = 512
TOKEN_COUNT = 4096
N_SEQ = 8


def draw_log_decay(key, part):
    every_key = jax.random.split(jax.random.fold_in(key, 7), 6)
    share = 0.5
    slow = jax.random.uniform(every_key[0], (HEAD_COUNT,)) < share
    slow_rate = jnp.exp(jax.random.uniform(every_key[1], (HEAD_COUNT,), jnp.float32, jnp.log(0.05), jnp.log(0.5))) / TOKEN_COUNT
    fast_rate = jax.random.uniform(every_key[2], (HEAD_COUNT,), jnp.float32, 1.0 / 50.0, 1.0 / 30.0)
    decay_rate = jnp.where(slow, slow_rate, fast_rate)
    random_noise = jax.random.uniform(every_key[3], (TOKEN_COUNT, HEAD_COUNT), jnp.float32, 0.5, 1.5)
    decay_spike = jax.random.uniform(every_key[4], (TOKEN_COUNT, HEAD_COUNT)) < 3.0 / TOKEN_COUNT
    decay_falloff = jnp.log(jax.random.uniform(every_key[5], (TOKEN_COUNT, HEAD_COUNT), jnp.float32, 0.5, 0.8))
    return (-decay_rate[None, :] * random_noise + jnp.where(decay_spike, decay_falloff, 0.0)).astype(jnp.float32)


def steps_of(key, shape, cuts, smallest, top_value):
    def one(position, parts):
        draws = jax.random.uniform(jax.random.fold_in(jax.random.fold_in(key, 6), position), (parts,), jnp.float32, smallest / len(cuts), top_value / len(cuts))
        return jnp.repeat(jnp.exp(draws), shape[position] // parts).reshape((-1,) + (1,) * (len(shape) - position - 1))

    loudness = one(*cuts[0])
    for cut in cuts[1:]:
        loudness = loudness * one(*cut)
    return loudness


def scatter_about(own_key, extent, scale, reach, cuts=(), dtype=jnp.bfloat16):
    drawn = scale * jax.random.normal(own_key, extent, jnp.float32)
    if cuts:
        drawn = drawn * steps_of(own_key, extent, cuts, -0.22, 0.18)
    return jnp.clip(drawn, -reach, reach).astype(dtype)


def setup_inputs(seed: int = 0) -> dict:
    key_of = jax.random.split(jax.random.key(seed), 7)
    queries = scatter_about(key_of[0], (TOKEN_COUNT, HEAD_COUNT * HEAD), 1.0, 6.0, ((0, 8), (1, 4)))
    keys = scatter_about(key_of[1], (TOKEN_COUNT, HEAD_COUNT * HEAD), HEAD ** -0.5, 0.5, ((0, 8), (1, 4)))
    values = scatter_about(key_of[2], (TOKEN_COUNT, HEAD_COUNT * HEAD), 1.0, 6.0, ((0, 8), (1, 4)))
    gate = scatter_about(key_of[3], (TOKEN_COUNT, HEAD_COUNT * HEAD), 1.0, 6.0, ((0, 8), (1, 4)))
    log_decay = draw_log_decay(jax.random.fold_in(key_of[6], 71), 0)
    out_grad = scatter_about(key_of[5], (TOKEN_COUNT, HEAD_COUNT * HEAD), 1.0, 6.0, ((0, 8), (1, 4)))
    return {"queries": queries, "keys": keys, "values": values, "gate": gate, "log_decay": log_decay, "out_grad": out_grad}


HIGH = lax.Precision.HIGHEST

def decay_table(within):
    gap = within.T[:, :, None] - within.T[:, None, :]
    rows = lax.broadcasted_iota(jnp.int32, gap.shape, 1)
    cols = lax.broadcasted_iota(jnp.int32, gap.shape, 2)
    return jnp.where(rows >= cols, jnp.exp(jnp.minimum(gap, 0.0)), 0.0)

def block_probs(qh, kh, decay):
    scores = jnp.einsum('thd,shd->hts', qh.astype(jnp.float32), kh.astype(jnp.float32))
    return (scores * decay).astype(jnp.bfloat16)

def forward_block(state, pieces):
    qh, kh, vh, rates = pieces
    within = jnp.cumsum(rates, axis=0)
    last = within[-1]
    decay = decay_table(within)
    probs = block_probs(qh, kh, decay)
    qf = qh.astype(jnp.float32)
    kf = kh.astype(jnp.float32)
    vf = vh.astype(jnp.float32)
    intra = jnp.einsum('hts,shd->thd', probs.astype(jnp.float32), vf)
    inter = jnp.exp(within)[:, :, None] * jnp.einsum('thd,hde->the', qf, state, precision=HIGH)
    tail = jnp.exp(last[None, :] - within)
    local = jnp.einsum('thd,the->hde', kf * tail[:, :, None], vf, precision=HIGH)
    fresh = jnp.exp(last)[:, None, None] * state + local
    return (fresh, (intra + inter, state))

def backward_block(grad_state, pieces):
    qh, kh, vh, rates, grad_b, state = pieces
    within = jnp.cumsum(rates, axis=0)
    last = within[-1]
    decay = decay_table(within)
    probs = block_probs(qh, kh, decay)
    qf = qh.astype(jnp.float32)
    kf = kh.astype(jnp.float32)
    vf = vh.astype(jnp.float32)
    gradf = grad_b.astype(jnp.float32)
    pgrad = (jnp.einsum('thd,shd->hts', gradf, vf) * decay).astype(jnp.bfloat16).astype(jnp.float32)
    grow = jnp.exp(within)[:, :, None]
    tail = jnp.exp(last[None, :] - within)[:, :, None]
    query_grad = jnp.einsum('hts,shd->thd', pgrad, kf) + grow * jnp.einsum('the,hde->thd', gradf, state, precision=HIGH)
    key_grad = jnp.einsum('hts,thd->shd', pgrad, qf) + tail * jnp.einsum('the,hde->thd', vf, grad_state, precision=HIGH)
    value_grad = jnp.einsum('hts,thd->shd', probs.astype(jnp.float32), gradf) + tail * jnp.einsum('thd,hde->the', kf, grad_state, precision=HIGH)
    weighted = jnp.einsum('thd,the->hde', qf * grow, gradf, precision=HIGH)
    fresh = weighted + jnp.exp(last)[:, None, None] * grad_state
    return (fresh, (query_grad.astype(jnp.bfloat16), key_grad.astype(jnp.bfloat16), value_grad.astype(jnp.bfloat16)))

def reference(queries, keys, values, gate, log_decay, out_grad):
    blocks = N_SEQ
    width = HEAD_COUNT * HEAD
    qb = queries.reshape(blocks, TOK_DEV, HEAD_COUNT, HEAD)
    kb = keys.reshape(blocks, TOK_DEV, HEAD_COUNT, HEAD)
    vb = values.reshape(blocks, TOK_DEV, HEAD_COUNT, HEAD)
    rb = log_decay.reshape(blocks, TOK_DEV, HEAD_COUNT)
    start = jnp.zeros((HEAD_COUNT, HEAD, HEAD), jnp.float32)
    unused, (attn_blocks, states) = lax.scan(forward_block, start, (qb, kb, vb, rb))
    attn = attn_blocks.reshape(TOKEN_COUNT, width)
    scale = lax.rsqrt(lax.optimization_barrier(jnp.sum(attn * attn, axis=1)) / width + 1e-06)
    normed = attn * scale[:, None]
    sig = jax.nn.sigmoid(gate.astype(jnp.float32))
    output = (normed * sig).astype(jnp.bfloat16)
    upstream = out_grad.astype(jnp.float32)
    dnorm = upstream * sig
    gate_grad = (upstream * normed * sig * (1.0 - sig)).astype(jnp.bfloat16)
    center = lax.optimization_barrier(jnp.sum(dnorm * normed, axis=1)) / width
    attn_grad = (scale[:, None] * (dnorm - normed * center[:, None])).astype(jnp.bfloat16)
    gb = attn_grad.reshape(blocks, TOK_DEV, HEAD_COUNT, HEAD)
    unused2, (dq, dk, dv) = lax.scan(backward_block, start, (qb, kb, vb, rb, gb, states), reverse=True)
    return (output, dq.reshape(TOKEN_COUNT, width), dk.reshape(TOKEN_COUNT, width), dv.reshape(TOKEN_COUNT, width), gate_grad)
```

```python
import functools

import jax
import jax.numpy as jnp
from jax import lax
from jax.experimental import pallas as pl
from jax.experimental.pallas import tpu as pltpu
from jax.sharding import PartitionSpec as P

MESH = pl.DeviceIdType.MESH
F32 = jnp.float32
BF16 = jnp.bfloat16
HIGH = lax.Precision.HIGHEST
EXTRA = 8
CHUNKS = 4


def nt(a, b):
    return lax.dot_general(a, b, (((1,), (1,)), ((), ())), preferred_element_type=F32)


def tn(a, b):
    return lax.dot_general(a, b, (((0,), (0,)), ((), ())), preferred_element_type=F32)


def nn(a, b):
    return lax.dot_general(a, b, (((1,), (0,)), ((), ())), preferred_element_type=F32)


def kernel(
    n_seq, n_tp, heads, dim, tokens,
    q_hbm, k_hbm, v_hbm, gate_hbm, rate_hbm, up_hbm,
    out_hbm, dq_hbm, dk_hbm, dv_hbm, gg_hbm,
    q, k, v, gate, rate, up, rates_wide, rows, cols, attn, dvp, grad, probs,
    own, other, sent, got, edge, far, state, sums, sums_in, scale_ref, center_ref,
    in_sem, out_sem, s0_send, s0_recv, st_send, st_recv, fin_send, fin_recv, tp_send, tp_recv,
):
    width = heads * dim * n_tp
    half = heads // 2
    bits = n_seq.bit_length() - 1
    chips = bits - 1
    per = half // CHUNKS
    block = min(256, tokens)
    nb = tokens // block
    me = lax.axis_index("seq")
    z = lax.axis_index("tp")
    core = lax.rem(me, 2)

    def bit_of(b):
        return lax.rem(me // (1 << b), 2)

    def partner(b):
        return (me + (1 << b) * (1 - 2 * bit_of(b)), z)

    def take(d, b):
        bit = bit_of(b).astype(F32)
        return bit if d == 0 else 1.0 - bit

    loads = []
    for i, (a, b) in enumerate(
        ((rate_hbm, rate), (k_hbm, k), (v_hbm, v), (q_hbm, q), (up_hbm, up), (gate_hbm, gate))
    ):
        c = pltpu.make_async_copy(a, b, in_sem.at[i])
        c.start()
        loads.append(c)

    barrier = pltpu.get_barrier_semaphore()
    for b in range(bits):
        pl.semaphore_signal(barrier, inc=1, device_id=partner(b), device_id_type=MESH)
    for d in range(1, n_tp):
        pl.semaphore_signal(
            barrier, inc=1, device_id=(me, lax.rem(z + d, n_tp)), device_id_type=MESH
        )

    def lane(h):
        return pl.ds(pl.multiple_of(h * dim, dim), dim)

    def pairs(body):
        @pl.loop(0, heads // 2)
        def _(i):
            body(2 * i)
            body(2 * i + 1)

    loads[0].wait()
    rates_wide[...] = jnp.zeros_like(rates_wide)
    rates_wide[:, 0:heads] = rate[...]
    tri = (
        lax.broadcasted_iota(jnp.int32, (tokens, tokens), 0)
        >= lax.broadcasted_iota(jnp.int32, (tokens, tokens), 1)
    ).astype(F32)
    within = lax.dot_general(
        tri, rates_wide[...], (((1,), (0,)), ((), ())), precision=HIGH, preferred_element_type=F32
    )
    rows[...] = within.T
    for h in range(heads):
        cols[h] = jnp.broadcast_to(within[:, h : h + 1], (tokens, dim))

    loads[1].wait()
    loads[2].wait()

    def make_local(h):
        last = cols[h, tokens - 1 : tokens, :]
        scaled = (k[:, lane(h)].astype(F32) * jnp.exp(last - cols[h])).astype(BF16)
        own[0, h, 0:dim, :] = tn(scaled, v[:, lane(h)])
        own[0, h, dim : dim + EXTRA, :] = jnp.broadcast_to(last, (EXTRA, dim))

    pairs(make_local)

    def s0_copy(d):
        return pltpu.make_async_remote_copy(
            src_ref=own.at[d], dst_ref=other.at[d], send_sem=s0_send.at[d],
            recv_sem=s0_recv.at[d], device_id=partner(0), device_id_type=MESH,
        )

    def st_copy(d, s, c):
        part = pl.ds(c * per, per)
        return pltpu.make_async_remote_copy(
            src_ref=sent.at[d, s, part], dst_ref=got.at[d, s, part], send_sem=st_send.at[d, s, c],
            recv_sem=st_recv.at[d, s, c], device_id=partner(s + 1), device_id_type=MESH,
        )

    def fin_copy(d, c):
        part = pl.ds(c * per, per)
        return pltpu.make_async_remote_copy(
            src_ref=edge.at[d, part], dst_ref=far.at[d, part], send_sem=fin_send.at[d, c],
            recv_sem=fin_recv.at[d, c], device_id=partner(0), device_id_type=MESH,
        )

    def joined(f, mine, theirs):
        dm, dt = mine[dim : dim + 1], theirs[dim : dim + 1]
        total = jnp.exp(dt * (1.0 - f)) * mine[0:dim] + jnp.exp(dm * f) * theirs[0:dim]
        return total, mine[dim:] + theirs[dim:]

    def step_first(d):
        s0_copy(d).wait_recv()
        f = take(d, 0)
        for c in range(CHUNKS):

            @pl.loop(0, per)
            def _(i):
                hh = c * per + i
                h = core * half + hh
                total, span = joined(f, own[d, h], other[d, h])
                sent[d, 0, hh, 0:dim, :] = total
                sent[d, 0, hh, dim:, :] = span
                edge[d, hh] = jnp.zeros((dim + EXTRA, dim), F32)

            if chips:
                st_copy(d, 0, c).start()
            else:
                fin_copy(d, c).start()

    def step(d, s, c):
        st_copy(d, s, c).wait_recv()
        f = take(d, s + 1)

        @pl.loop(0, per)
        def _(i):
            hh = c * per + i
            theirs = got[d, s, hh]
            e = edge[d, hh, dim : dim + 1, :]
            edge[d, hh, 0:dim, :] = edge[d, hh, 0:dim, :] + (f * jnp.exp(e)) * theirs[0:dim]
            edge[d, hh, dim:, :] = edge[d, hh, dim:, :] + f * theirs[dim:]
            if s + 1 < chips:
                total, span = joined(f, sent[d, s, hh], theirs)
                sent[d, s + 1, hh, 0:dim, :] = total
                sent[d, s + 1, hh, dim:, :] = span

        if s + 1 < chips:
            st_copy(d, s + 1, c).start()
        else:
            fin_copy(d, c).start()

    def step_last(d):
        f = take(d, 0)

        def put(h, e):
            span = other[d, h, dim : dim + 1, :]
            state[d, h] = (jnp.exp(span * f) * e + f * other[d, h, 0:dim, :]).astype(BF16)

        @pl.loop(0, half)
        def _(hh):
            put(core * half + hh, edge[d, hh, 0:dim, :])

        for c in range(CHUNKS):
            fin_copy(d, c).wait_recv()

            @pl.loop(0, per)
            def _(i):
                hh = c * per + i
                put((1 - core) * half + hh, far[d, hh, 0:dim, :])

    order = sorted(((s, c) for s in range(chips) for c in range(CHUNKS)), key=lambda p: (2 * p[0] + p[1], p[0]))

    def exchange_beside(d, body):
        trips = heads // 2
        s0_copy(d).start()
        early = min(2, trips)
        inside = order[: max(0, (trips - early) // 2)]

        @pl.loop(0, trips)
        def _(i):
            body(2 * i)
            body(2 * i + 1)

            @pl.when(i == early - 1)
            def _():
                step_first(d)

            for n, (s, c) in enumerate(inside):

                @pl.when(i == early + 2 * n + 1)
                def _():
                    step(d, s, c)

        for s, c in order[len(inside) :]:
            step(d, s, c)
        step_last(d)

    tiles = [(i, j) for i in range(nb) for j in range(i + 1)]
    keep = (
        lax.broadcasted_iota(jnp.int32, (block, block), 0)
        >= lax.broadcasted_iota(jnp.int32, (block, block), 1)
    )

    def decay_of(h, i, j):
        col = cols[h, i * block : (i + 1) * block, :]
        col = jnp.concatenate([col] * (block // dim), axis=1)
        row = rows[pl.ds(h, 1), j * block : (j + 1) * block]
        value = jnp.exp(jnp.minimum(col - row, 0.0))
        return jnp.where(keep, value, 0.0) if i == j else value

    def span_of(i):
        return slice(i * block, (i + 1) * block)

    def intra(h):
        for i in range(nb):
            total = None
            for j in range(i + 1):
                s = nt(q[span_of(i), lane(h)], k[span_of(j), lane(h)])
                p = (s * decay_of(h, i, j)).astype(BF16)
                probs[h, tiles.index((i, j))] = p
                o = nn(p, v[span_of(j), lane(h)])
                total = o if total is None else total + o
            attn[span_of(i), lane(h)] = total

    loads[3].wait()
    pl.semaphore_wait(barrier, bits + n_tp - 1)
    exchange_beside(0, intra)

    loads[4].wait()
    loads[5].wait()
    scale_ref[...] = jnp.zeros_like(scale_ref)
    center_ref[...] = jnp.zeros_like(center_ref)

    def finish_attn(h):
        for i in range(nb):
            r = span_of(i)
            a = attn[r, lane(h)] + jnp.exp(cols[h, r, :]) * nn(q[r, lane(h)], state[0, h])
            attn[r, lane(h)] = a
            scale_ref[r, :] = scale_ref[r, :] + a * a
            sig = jax.nn.sigmoid(gate[r, lane(h)].astype(F32))
            center_ref[r, :] = center_ref[r, :] + up[r, lane(h)].astype(F32) * sig * a

    pairs(finish_attn)

    ones = jnp.ones((8, dim), F32)

    def lanes_summed(x):
        return lax.dot_general(
            ones, x, (((1,), (1,)), ((), ())), precision=HIGH, preferred_element_type=F32
        )

    sums[0:8, :] = lanes_summed(scale_ref[...])
    sums[8:16, :] = lanes_summed(center_ref[...])

    def tp_copy(d):
        return pltpu.make_async_remote_copy(
            src_ref=sums, dst_ref=sums_in.at[d - 1], send_sem=tp_send.at[d - 1],
            recv_sem=tp_recv.at[d - 1], device_id=(me, lax.rem(z + d, n_tp)), device_id_type=MESH,
        )

    for d in range(1, n_tp):
        tp_copy(d).start()
    total = sums[...]
    for d in range(1, n_tp):
        tp_copy(d).wait_recv()
        total = total + sums_in[d - 1]

    def spread(x):
        return lax.dot_general(
            x, ones / 8.0, (((0,), (0,)), ((), ())), precision=HIGH, preferred_element_type=F32
        )

    scale = lax.rsqrt(spread(total[0:8]) / width + 1e-06)
    scale_ref[...] = scale
    center_ref[...] = spread(total[8:16]) * scale / width

    def pointwise(h):
        weighted = None
        for i in range(nb):
            r = span_of(i)
            sc = scale_ref[r, :]
            normed = attn[r, lane(h)] * sc
            sig = jax.nn.sigmoid(gate[r, lane(h)].astype(F32))
            dnorm = up[r, lane(h)].astype(F32) * sig
            g = (sc * (dnorm - normed * center_ref[r, :])).astype(BF16)
            grad[r, lane(h)] = g
            up[r, lane(h)] = (normed * sig).astype(BF16)
            gate[r, lane(h)] = (dnorm * normed * (1.0 - sig)).astype(BF16)
            grown = (q[r, lane(h)].astype(F32) * jnp.exp(cols[h, r, :])).astype(BF16)
            w = tn(grown, g)
            weighted = w if weighted is None else weighted + w
        own[1, h, 0:dim, :] = weighted
        own[1, h, dim : dim + EXTRA, :] = own[0, h, dim : dim + EXTRA, :]

    pairs(pointwise)

    outs = [
        pltpu.make_async_copy(a, b, out_sem.at[i])
        for i, (a, b) in enumerate(
            ((up, out_hbm), (gate, gg_hbm), (q, dq_hbm), (k, dk_hbm), (v, dv_hbm))
        )
    ]
    outs[0].start()
    outs[1].start()

    def backward(h):
        dq = [None] * nb
        dk = [None] * nb
        dv = [None] * nb

        def add(parts, n, x):
            parts[n] = x if parts[n] is None else parts[n] + x

        for i, j in tiles:
            g = grad[span_of(i), lane(h)]
            pg = (nt(g, v[span_of(j), lane(h)]) * decay_of(h, i, j)).astype(BF16)
            add(dq, i, nn(pg, k[span_of(j), lane(h)]))
            add(dk, j, tn(pg, q[span_of(i), lane(h)]))
            add(dv, j, tn(probs[h, tiles.index((i, j))], g))
        for i in range(nb):
            r = span_of(i)
            carried = jnp.exp(cols[h, r, :]) * nt(grad[r, lane(h)], state[0, h])
            q[r, lane(h)] = (dq[i] + carried).astype(BF16)
            attn[r, lane(h)] = dk[i]
            dvp[r, lane(h)] = dv[i]

    exchange_beside(1, backward)
    outs[2].start()

    def finish(h):
        last = cols[h, tokens - 1 : tokens, :]
        for i in range(nb):
            r = span_of(i)
            tail = jnp.exp(last - cols[h, r, :])
            kk, vv = k[r, lane(h)], v[r, lane(h)]
            dk = attn[r, lane(h)] + tail * nt(vv, state[1, h])
            dv = dvp[r, lane(h)] + tail * nn(kk, state[1, h])
            k[r, lane(h)] = dk.astype(BF16)
            v[r, lane(h)] = dv.astype(BF16)

    pairs(finish)
    outs[3].start()
    outs[4].start()

    for d in (0, 1):
        s0_copy(d).wait_send()
        for c in range(CHUNKS):
            for s in range(chips):
                st_copy(d, s, c).wait_send()
            fin_copy(d, c).wait_send()
    for d in range(1, n_tp):
        tp_copy(d).wait_send()
    for c in outs:
        c.wait()


def solution(mesh):
    n_seq, n_tp = mesh.shape["seq"], mesh.shape["tp"]

    def shards(queries, keys, values, gate, log_decay, out_grad):
        tokens, flat = queries.shape
        heads = log_decay.shape[1]
        dim = flat // heads
        half = heads // 2
        chips = n_seq.bit_length() - 2
        block = min(256, tokens)
        nb = tokens // block
        big = pltpu.VMEM((tokens, flat), BF16)
        wide = pltpu.VMEM((tokens, flat), F32)
        message = (dim + EXTRA, dim)
        dma = pltpu.SemaphoreType.DMA
        any_spec = pl.BlockSpec(memory_space=pl.ANY)
        flops = 2 * tokens * tokens * flat * 5 + 2 * tokens * flat * dim * 7
        return tuple(
            pl.pallas_call(
                functools.partial(kernel, n_seq, n_tp, heads, dim, tokens),
                out_shape=[jax.ShapeDtypeStruct((tokens, flat), BF16)] * 5,
                in_specs=[any_spec] * 6,
                out_specs=[any_spec] * 5,
                scratch_shapes=[
                    big, big, big, big, pltpu.VMEM((tokens, heads), F32), big,
                    pltpu.VMEM((tokens, 128), F32), pltpu.VMEM((128, tokens), F32),
                    pltpu.VMEM((heads, tokens, dim), F32), wide, wide, big,
                    pltpu.VMEM((heads, nb * (nb + 1) // 2, block, block), BF16),
                    pltpu.VMEM((2, heads, *message), F32),
                    pltpu.VMEM((2, heads, *message), F32),
                    pltpu.VMEM((2, max(chips, 1), half, *message), F32),
                    pltpu.VMEM((2, max(chips, 1), half, *message), F32),
                    pltpu.VMEM((2, half, *message), F32),
                    pltpu.VMEM((2, half, *message), F32),
                    pltpu.VMEM((2, heads, dim, dim), BF16),
                    pltpu.VMEM((16, tokens), F32),
                    pltpu.VMEM((max(n_tp - 1, 1), 16, tokens), F32),
                    pltpu.VMEM((tokens, dim), F32), pltpu.VMEM((tokens, dim), F32),
                    dma((6,)), dma((5,)), dma((2,)), dma((2,)),
                    dma((2, max(chips, 1), CHUNKS)), dma((2, max(chips, 1), CHUNKS)),
                    dma((2, CHUNKS)), dma((2, CHUNKS)),
                    dma((max(n_tp - 1, 1),)), dma((max(n_tp - 1, 1),)),
                ],
                compiler_params=pltpu.CompilerParams(
                    collective_id=0, has_side_effects=True, vmem_limit_bytes=58 << 20
                ),
                cost_estimate=pl.CostEstimate(
                    flops=flops, bytes_accessed=tokens * flat * 20, transcendentals=0
                ),
            )(queries, keys, values, gate, log_decay, out_grad)
        )

    spec = P("seq", "tp")
    return jax.shard_map(
        shards, mesh=mesh, in_specs=(spec,) * 6, out_specs=(spec,) * 5, check_vma=False
    )
```

```python
import functools

import jax
import jax.numpy as jnp
from jax import lax
from jax.experimental import pallas as pl
from jax.experimental.pallas import tpu as pltpu
from jax.sharding import PartitionSpec as P

MESH = pl.DeviceIdType.MESH
F32 = jnp.float32
BF16 = jnp.bfloat16
HIGH = lax.Precision.HIGHEST
EXTRA = 8
CHUNKS = 4


def nt(a, b):
    return lax.dot_general(a, b, (((1,), (1,)), ((), ())), preferred_element_type=F32)


def tn(a, b):
    return lax.dot_general(a, b, (((0,), (0,)), ((), ())), preferred_element_type=F32)


def nn(a, b):
    return lax.dot_general(a, b, (((1,), (0,)), ((), ())), preferred_element_type=F32)


def kernel(
    n_seq, n_tp, heads, dim, tokens,
    q_hbm, k_hbm, v_hbm, gate_hbm, rate_hbm, up_hbm,
    out_hbm, dq_hbm, dk_hbm, dv_hbm, gg_hbm,
    q, k, v, gate, rate, up, rates_wide, rows, cols, attn, dvp, grad, probs,
    own, other, sent, got, edge, far, state, sums, sums_in, scale_ref, center_ref,
    in_sem, out_sem, s0_send, s0_recv, st_send, st_recv, fin_send, fin_recv, tp_send, tp_recv,
):
    width = heads * dim * n_tp
    half = heads // 2
    bits = n_seq.bit_length() - 1
    chips = bits - 1
    per = half // CHUNKS
    block = min(256, tokens)
    nb = tokens // block
    me = lax.axis_index("seq")
    z = lax.axis_index("tp")
    core = lax.rem(me, 2)

    def bit_of(b):
        return lax.rem(me // (1 << b), 2)

    def partner(b):
        return (me + (1 << b) * (1 - 2 * bit_of(b)), z)

    def take(d, b):
        bit = bit_of(b).astype(F32)
        return bit if d == 0 else 1.0 - bit

    loads = []
    for i, (a, b) in enumerate(
        ((rate_hbm, rate), (k_hbm, k), (v_hbm, v), (q_hbm, q), (up_hbm, up), (gate_hbm, gate))
    ):
        c = pltpu.make_async_copy(a, b, in_sem.at[i])
        c.start()
        loads.append(c)

    barrier = pltpu.get_barrier_semaphore()
    for b in range(bits):
        pl.semaphore_signal(barrier, inc=1, device_id=partner(b), device_id_type=MESH)
    for d in range(1, n_tp):
        pl.semaphore_signal(
            barrier, inc=1, device_id=(me, lax.rem(z + d, n_tp)), device_id_type=MESH
        )

    def lane(h):
        return pl.ds(pl.multiple_of(h * dim, dim), dim)

    def pairs(body):
        @pl.loop(0, heads // 2)
        def _(i):
            body(2 * i)
            body(2 * i + 1)

    loads[0].wait()
    rates_wide[...] = jnp.zeros_like(rates_wide)
    rates_wide[0:heads, :] = rate[...]
    tri = (
        lax.broadcasted_iota(jnp.int32, (tokens, tokens), 0)
        >= lax.broadcasted_iota(jnp.int32, (tokens, tokens), 1)
    ).astype(F32)
    across = lax.dot_general(
        rates_wide[...], tri, (((1,), (1,)), ((), ())), precision=HIGH, preferred_element_type=F32
    )
    rows[...] = across
    within = across.T
    for h in range(heads):
        cols[h] = jnp.broadcast_to(within[:, h : h + 1], (tokens, dim))

    loads[1].wait()
    loads[2].wait()

    def make_local(h):
        last = cols[h, tokens - 1 : tokens, :]
        scaled = (k[:, lane(h)].astype(F32) * jnp.exp(last - cols[h])).astype(BF16)
        own[0, h, 0:dim, :] = tn(scaled, v[:, lane(h)])
        own[0, h, dim : dim + EXTRA, :] = jnp.broadcast_to(last, (EXTRA, dim))

    pairs(make_local)

    def s0_copy(d):
        return pltpu.make_async_remote_copy(
            src_ref=own.at[d], dst_ref=other.at[d], send_sem=s0_send.at[d],
            recv_sem=s0_recv.at[d], device_id=partner(0), device_id_type=MESH,
        )

    def st_copy(d, s, c):
        part = pl.ds(c * per, per)
        return pltpu.make_async_remote_copy(
            src_ref=sent.at[d, s, part], dst_ref=got.at[d, s, part], send_sem=st_send.at[d, s, c],
            recv_sem=st_recv.at[d, s, c], device_id=partner(s + 1), device_id_type=MESH,
        )

    def fin_copy(d, c):
        part = pl.ds(c * per, per)
        return pltpu.make_async_remote_copy(
            src_ref=edge.at[d, part], dst_ref=far.at[d, part], send_sem=fin_send.at[d, c],
            recv_sem=fin_recv.at[d, c], device_id=partner(0), device_id_type=MESH,
        )

    def joined(f, mine, theirs):
        dm, dt = mine[dim : dim + 1], theirs[dim : dim + 1]
        total = jnp.exp(dt * (1.0 - f)) * mine[0:dim] + jnp.exp(dm * f) * theirs[0:dim]
        return total, mine[dim:] + theirs[dim:]

    def step_first(d):
        s0_copy(d).wait_recv()
        f = take(d, 0)
        for c in range(CHUNKS):

            @pl.loop(0, per)
            def _(i):
                hh = c * per + i
                h = core * half + hh
                total, span = joined(f, own[d, h], other[d, h])
                sent[d, 0, hh, 0:dim, :] = total
                sent[d, 0, hh, dim:, :] = span
                edge[d, hh] = jnp.zeros((dim + EXTRA, dim), F32)

            if chips:
                st_copy(d, 0, c).start()
            else:
                fin_copy(d, c).start()

    def step(d, s, c):
        st_copy(d, s, c).wait_recv()
        f = take(d, s + 1)

        @pl.loop(0, per)
        def _(i):
            hh = c * per + i
            theirs = got[d, s, hh]
            e = edge[d, hh, dim : dim + 1, :]
            edge[d, hh, 0:dim, :] = edge[d, hh, 0:dim, :] + (f * jnp.exp(e)) * theirs[0:dim]
            edge[d, hh, dim:, :] = edge[d, hh, dim:, :] + f * theirs[dim:]
            if s + 1 < chips:
                total, span = joined(f, sent[d, s, hh], theirs)
                sent[d, s + 1, hh, 0:dim, :] = total
                sent[d, s + 1, hh, dim:, :] = span

        if s + 1 < chips:
            st_copy(d, s + 1, c).start()
        else:
            fin_copy(d, c).start()

    def step_last(d):
        f = take(d, 0)

        def put(h, e):
            span = other[d, h, dim : dim + 1, :]
            state[d, h] = (jnp.exp(span * f) * e + f * other[d, h, 0:dim, :]).astype(BF16)

        @pl.loop(0, half)
        def _(hh):
            put(core * half + hh, edge[d, hh, 0:dim, :])

        for c in range(CHUNKS):
            fin_copy(d, c).wait_recv()

            @pl.loop(0, per)
            def _(i):
                hh = c * per + i
                put((1 - core) * half + hh, far[d, hh, 0:dim, :])

    order = sorted(((s, c) for s in range(chips) for c in range(CHUNKS)), key=lambda p: (2 * p[0] + p[1], p[0]))

    def exchange_beside(d, body):
        trips = heads // 2
        s0_copy(d).start()
        early = min(2, trips)
        inside = order[: max(0, (trips - early) // 2)]

        @pl.loop(0, trips)
        def _(i):
            body(2 * i)
            body(2 * i + 1)

            @pl.when(i == early - 1)
            def _():
                step_first(d)

            for n, (s, c) in enumerate(inside):

                @pl.when(i == early + 2 * n + 1)
                def _():
                    step(d, s, c)

        for s, c in order[len(inside) :]:
            step(d, s, c)
        step_last(d)

    tiles = [(i, j) for i in range(nb) for j in range(i + 1)]
    keep = (
        lax.broadcasted_iota(jnp.int32, (block, block), 0)
        >= lax.broadcasted_iota(jnp.int32, (block, block), 1)
    )

    def decay_of(h, i, j):
        col = cols[h, i * block : (i + 1) * block, :]
        col = jnp.concatenate([col] * (block // dim), axis=1)
        row = rows[pl.ds(h, 1), j * block : (j + 1) * block]
        value = jnp.exp(jnp.minimum(col - row, 0.0))
        return jnp.where(keep, value, 0.0) if i == j else value

    def span_of(i):
        return slice(i * block, (i + 1) * block)

    def intra(h):
        for i in range(nb):
            total = None
            for j in range(i + 1):
                s = nt(q[span_of(i), lane(h)], k[span_of(j), lane(h)])
                p = (s * decay_of(h, i, j)).astype(BF16)
                probs[h, tiles.index((i, j))] = p
                o = nn(p, v[span_of(j), lane(h)])
                total = o if total is None else total + o
            attn[span_of(i), lane(h)] = total

    loads[3].wait()
    pl.semaphore_wait(barrier, bits + n_tp - 1)
    exchange_beside(0, intra)

    loads[4].wait()
    loads[5].wait()
    scale_ref[...] = jnp.zeros_like(scale_ref)
    center_ref[...] = jnp.zeros_like(center_ref)

    def finish_attn(h):
        for i in range(nb):
            r = span_of(i)
            a = attn[r, lane(h)] + jnp.exp(cols[h, r, :]) * nn(q[r, lane(h)], state[0, h])
            attn[r, lane(h)] = a
            scale_ref[r, :] = scale_ref[r, :] + a * a
            sig = jax.nn.sigmoid(gate[r, lane(h)].astype(F32))
            center_ref[r, :] = center_ref[r, :] + up[r, lane(h)].astype(F32) * sig * a

    pairs(finish_attn)

    ones = jnp.ones((8, dim), F32)

    def lanes_summed(x):
        return lax.dot_general(
            ones, x, (((1,), (1,)), ((), ())), precision=HIGH, preferred_element_type=F32
        )

    sums[0:8, :] = lanes_summed(scale_ref[...])
    sums[8:16, :] = lanes_summed(center_ref[...])

    def tp_copy(d):
        return pltpu.make_async_remote_copy(
            src_ref=sums, dst_ref=sums_in.at[d - 1], send_sem=tp_send.at[d - 1],
            recv_sem=tp_recv.at[d - 1], device_id=(me, lax.rem(z + d, n_tp)), device_id_type=MESH,
        )

    for d in range(1, n_tp):
        tp_copy(d).start()
    total = sums[...]
    for d in range(1, n_tp):
        tp_copy(d).wait_recv()
        total = total + sums_in[d - 1]

    def spread(x):
        return lax.dot_general(
            x, ones / 8.0, (((0,), (0,)), ((), ())), precision=HIGH, preferred_element_type=F32
        )

    scale = lax.rsqrt(spread(total[0:8]) / width + 1e-06)
    scale_ref[...] = scale
    center_ref[...] = spread(total[8:16]) * scale / width

    def pointwise(h):
        weighted = None
        for i in range(nb):
            r = span_of(i)
            sc = scale_ref[r, :]
            normed = attn[r, lane(h)] * sc
            sig = jax.nn.sigmoid(gate[r, lane(h)].astype(F32))
            dnorm = up[r, lane(h)].astype(F32) * sig
            g = (sc * (dnorm - normed * center_ref[r, :])).astype(BF16)
            grad[r, lane(h)] = g
            up[r, lane(h)] = (normed * sig).astype(BF16)
            gate[r, lane(h)] = (dnorm * normed * (1.0 - sig)).astype(BF16)
            grown = (q[r, lane(h)].astype(F32) * jnp.exp(cols[h, r, :])).astype(BF16)
            w = tn(grown, g)
            weighted = w if weighted is None else weighted + w
        own[1, h, 0:dim, :] = weighted
        own[1, h, dim : dim + EXTRA, :] = own[0, h, dim : dim + EXTRA, :]

    pairs(pointwise)

    outs = [
        pltpu.make_async_copy(a, b, out_sem.at[i])
        for i, (a, b) in enumerate(
            ((up, out_hbm), (gate, gg_hbm), (q, dq_hbm), (k, dk_hbm), (v, dv_hbm))
        )
    ]
    outs[0].start()
    outs[1].start()

    def backward(h):
        dq = [None] * nb
        dk = [None] * nb
        dv = [None] * nb

        def add(parts, n, x):
            parts[n] = x if parts[n] is None else parts[n] + x

        for i, j in tiles:
            g = grad[span_of(i), lane(h)]
            pg = (nt(g, v[span_of(j), lane(h)]) * decay_of(h, i, j)).astype(BF16)
            add(dq, i, nn(pg, k[span_of(j), lane(h)]))
            add(dk, j, tn(pg, q[span_of(i), lane(h)]))
            add(dv, j, tn(probs[h, tiles.index((i, j))], g))
        for i in range(nb):
            r = span_of(i)
            carried = jnp.exp(cols[h, r, :]) * nt(grad[r, lane(h)], state[0, h])
            q[r, lane(h)] = (dq[i] + carried).astype(BF16)
            attn[r, lane(h)] = dk[i]
            dvp[r, lane(h)] = dv[i]

    exchange_beside(1, backward)
    outs[2].start()

    def finish(h):
        last = cols[h, tokens - 1 : tokens, :]
        for i in range(nb):
            r = span_of(i)
            tail = jnp.exp(last - cols[h, r, :])
            kk, vv = k[r, lane(h)], v[r, lane(h)]
            dk = attn[r, lane(h)] + tail * nt(vv, state[1, h])
            dv = dvp[r, lane(h)] + tail * nn(kk, state[1, h])
            k[r, lane(h)] = dk.astype(BF16)
            v[r, lane(h)] = dv.astype(BF16)

    pairs(finish)
    outs[3].start()
    outs[4].start()

    for d in (0, 1):
        s0_copy(d).wait_send()
        for c in range(CHUNKS):
            for s in range(chips):
                st_copy(d, s, c).wait_send()
            fin_copy(d, c).wait_send()
    for d in range(1, n_tp):
        tp_copy(d).wait_send()
    for c in outs:
        c.wait()


def hand_on(*refs):
    for source, target in zip(refs[:5], refs[5:]):
        target[...] = source[...]


def solution(mesh):
    n_seq, n_tp = mesh.shape["seq"], mesh.shape["tp"]

    def shards(queries, keys, values, gate, log_decay, out_grad):
        tokens, flat = queries.shape
        heads = log_decay.shape[1]
        dim = flat // heads
        half = heads // 2
        chips = n_seq.bit_length() - 2
        block = min(256, tokens)
        nb = tokens // block
        big = pltpu.VMEM((tokens, flat), BF16)
        wide = pltpu.VMEM((tokens, flat), F32)
        message = (dim + EXTRA, dim)
        dma = pltpu.SemaphoreType.DMA
        any_spec = pl.BlockSpec(memory_space=pl.ANY)
        flops = 2 * tokens * tokens * flat * 5 + 2 * tokens * flat * dim * 7
        results = tuple(
            pl.pallas_call(
                functools.partial(kernel, n_seq, n_tp, heads, dim, tokens),
                out_shape=[jax.ShapeDtypeStruct((tokens, flat), BF16)] * 5,
                in_specs=[any_spec] * 6,
                out_specs=[any_spec] * 5,
                scratch_shapes=[
                    big, big, big, big, pltpu.VMEM((heads, tokens), F32), big,
                    pltpu.VMEM((128, tokens), F32), pltpu.VMEM((128, tokens), F32),
                    pltpu.VMEM((heads, tokens, dim), F32), wide, wide, big,
                    pltpu.VMEM((heads, nb * (nb + 1) // 2, block, block), BF16),
                    pltpu.VMEM((2, heads, *message), F32),
                    pltpu.VMEM((2, heads, *message), F32),
                    pltpu.VMEM((2, max(chips, 1), half, *message), F32),
                    pltpu.VMEM((2, max(chips, 1), half, *message), F32),
                    pltpu.VMEM((2, half, *message), F32),
                    pltpu.VMEM((2, half, *message), F32),
                    pltpu.VMEM((2, heads, dim, dim), BF16),
                    pltpu.VMEM((16, tokens), F32),
                    pltpu.VMEM((max(n_tp - 1, 1), 16, tokens), F32),
                    pltpu.VMEM((tokens, dim), F32), pltpu.VMEM((tokens, dim), F32),
                    dma((6,)), dma((5,)), dma((2,)), dma((2,)),
                    dma((2, max(chips, 1), CHUNKS)), dma((2, max(chips, 1), CHUNKS)),
                    dma((2, CHUNKS)), dma((2, CHUNKS)),
                    dma((max(n_tp - 1, 1),)), dma((max(n_tp - 1, 1),)),
                ],
                compiler_params=pltpu.CompilerParams(
                    collective_id=0, has_side_effects=True, vmem_limit_bytes=58 << 20
                ),
                cost_estimate=pl.CostEstimate(
                    flops=flops, bytes_accessed=tokens * flat * 20, transcendentals=0
                ),
            )(queries, keys, values, gate, log_decay.T, out_grad)
        )
        strip = pl.BlockSpec((tokens, flat // 4), lambda i: (0, i))
        return tuple(
            pl.pallas_call(
                hand_on,
                grid=(4,),
                out_shape=[jax.ShapeDtypeStruct((tokens, flat), BF16)] * 5,
                in_specs=[strip] * 5,
                out_specs=[strip] * 5,
            )(*results)
        )

    spec = P("seq", "tp")
    return jax.shard_map(
        shards, mesh=mesh, in_specs=(spec,) * 6, out_specs=(spec,) * 5, check_vma=False
    )
```
